32 devices in a mesh: dp: 4 (over x, core), vocab: 8 (over z, y).
Axes of the slice: x: 2, y: 2, z: 4, core: 2. Of those that a mesh axis runs over, the one named last changes fastest.
Arguments:
- hidden: bfloat16 [512, 8192], P('dp'), may hold values from -600 to 600
- out_weight: bfloat16 [8192, 98304], P('dp', 'vocab'), may hold values from -0.5 to 0.5
- targets: int32 [512], P('dp'), may hold values from 0 to 98303
- segment: int32 [512], P('dp'), may hold values from 0 to 15, never falling along the last dimension, each value on 1 to 64 neighbouring positions
- loss_mask: int32 [512], P('dp'), may hold values 0 or 1
- outside_count: int32 [16], replicated, may hold values from 0 to 3
Outputs:
- token_loss: float32 [512], P('dp')
- sample_loss: float32 [16], replicated
The draws below stay inside these ranges and needn't reach their ends.
All inputs are finite; a program needn't handle non-finite values. No bound on the sum of `loss_mask` on one device may be relied on, other than what follows from the above.
Results may differ from the reference program's by a relative error of at most 0.0003.
Values may be sent and summed in bfloat16 or wider, within the bound.
A program may use at most 128 MiB of HBM per device.

```python
import math
import jax
import jax.numpy as jnp
import numpy as np
from jax import lax

D = 8192
V = 98304
TOKENS = 512
SAMPLES = 16
SEG_MOST = 64


def weight_full(key):
    base = jax.random.normal(jax.random.fold_in(key, 7), (D, V), jnp.float32) * D ** (-0.5)
    return base


def draw_out_weight(key, part):
    return weight_full(key).astype(jnp.bfloat16)


def draw_hidden(key, part):
    states = jax.random.normal(jax.random.fold_in(key, 21), (TOKENS, D), jnp.float32) * 3.0
    return states.astype(jnp.bfloat16)


def set_ends(entries, key, smallest, top_value):
    index_at = [jax.random.randint(jax.random.fold_in(key, axis), (), 0, length) for axis, length in enumerate(entries.shape)]
    longest = entries.shape.index(max(entries.shape))
    neighbour = index_at[:longest] + [(index_at[longest] + 1) % entries.shape[longest]] + index_at[longest + 1:]
    return entries.at[tuple(index_at)].set(smallest).at[tuple(neighbour)].set(top_value)


def ranked_wide(stream_key, shape, number_of, slope):
    portions = [min(1 << octave, number_of + 1 - (1 << octave)) * (1 << 20) // math.isqrt((1 << octave) ** slope) + 1 for octave in range((number_of + 1).bit_length()) if 1 << octave <= number_of]
    spread = 1 + sum(portions) // (1 << 30)
    grid = np.cumsum(np.array([max(1, weight // spread) for weight in portions]))
    lot = jax.random.randint(jax.random.fold_in(stream_key, 1), shape, 0, int(grid[len(portions) - 1]))
    start = jnp.left_shift(1, jnp.searchsorted(jnp.asarray(grid, jnp.int32), lot, side="right").astype(jnp.int32))
    standing = start - 1 + jax.random.randint(jax.random.fold_in(stream_key, 4), shape, 0, 1 << 30) % jnp.minimum(start, number_of + 1 - start)
    return jax.random.permutation(jax.random.fold_in(stream_key, 2), number_of)[standing].astype(jnp.int32)


def length_profile(amount, total, reach, skew):
    weights = [(1 << 20) // math.isqrt(standing ** skew) + 1 for standing in range(2, amount + 1)]
    surplus, holding = total - reach - (amount - 1), [1] * (amount - 1)
    while surplus > 0:
        candidates = [i for i in range(amount - 1) if holding[i] < reach]
        pool, left = sum([weights[i] for i in candidates]), surplus
        for i in candidates:
            extra = min(reach - holding[i], max(1, left * weights[i] // pool), surplus)
            holding[i] = holding[i] + extra
            surplus = surplus - extra
    return np.array([reach] + holding)


def uneven(rng, number_of, total, reach, skew):
    if number_of == 2:
        one = jax.random.randint(rng, (), max(1, total - reach), min(reach, total - 1) + 1)
        return jnp.stack([one, total - one])
    lengths = jnp.asarray(length_profile(number_of, total, reach, skew), jnp.int32)
    couples = (number_of - 1) // 2
    donor, receiver = lengths[1:1 + 2 * couples:2], lengths[2:2 + 2 * couples:2]
    slack = jnp.minimum(donor - 1, reach - receiver)
    moved = jax.random.randint(jax.random.fold_in(rng, 1), (couples,), 0, 1 << 20) % (slack + 1)
    lengths = lengths.at[1:1 + 2 * couples:2].set(donor - moved).at[2:2 + 2 * couples:2].set(receiver + moved)
    return lengths[jax.random.permutation(jax.random.fold_in(rng, 2), number_of)]


def setup_inputs(seed: int = 0) -> dict:
    seeds = jax.random.split(jax.random.key(seed), 7)
    return {
        "hidden": draw_hidden(jax.random.fold_in(seeds[6], 71), 0),
        "out_weight": draw_out_weight(jax.random.fold_in(seeds[6], 71), 0),
        "targets": set_ends(ranked_wide(seeds[2], (TOKENS,), V, 2), jax.random.fold_in(seeds[2], 3), 0, V - 1).astype(jnp.int32),
        "segment": jnp.searchsorted(jnp.cumsum(uneven(seeds[3], SAMPLES, TOKENS, SEG_MOST, 2)), jnp.arange(TOKENS), side="right").astype(jnp.int32),
        "loss_mask": set_ends((jax.random.randint(seeds[4], (TOKENS,), 0, 4) < 3).astype(jnp.int32), jax.random.fold_in(seeds[4], 1), 0, 1),
        "outside_count": set_ends(jax.random.randint(seeds[5], (SAMPLES,), 0, 4), jax.random.fold_in(seeds[5], 1), 0, 3).astype(jnp.int32),
    }


def reference(hidden, out_weight, targets, segment, loss_mask, outside_count):
    block_rows = math.gcd(TOKENS, 256)
    block_count = TOKENS // block_rows
    hidden_blocks = hidden.reshape(block_count, block_rows, D)
    target_blocks = targets.reshape(block_count, block_rows)

    def one_block(pair):
        rows_block, target_block = pair
        logits = jnp.dot(rows_block, out_weight, preferred_element_type=jnp.float32)
        largest = jnp.max(logits, axis=1)
        lse = largest + jnp.log(jnp.sum(jnp.exp(logits - largest[:, None]), axis=1))
        picked = jnp.take_along_axis(logits, target_block[:, None].astype(jnp.int32), axis=1)[:, 0]
        return lse - picked

    token_loss = lax.map(one_block, (hidden_blocks, target_blocks)).reshape(TOKENS)
    onehot = (segment[:, None] == jnp.arange(SAMPLES, dtype=jnp.int32)[None, :]).astype(jnp.float32)
    weights = loss_mask.astype(jnp.float32)
    loss_sum = jnp.dot(token_loss * weights, onehot, precision=lax.Precision.HIGHEST)
    count = jnp.dot(weights, onehot, precision=lax.Precision.HIGHEST)
    denom = jnp.maximum(count + outside_count.astype(jnp.float32), 1.0)
    return token_loss, loss_sum / denom
```

```python
import functools

import jax
import jax.numpy as jnp
from jax import lax
from jax.experimental import pallas as pl
from jax.experimental.pallas import tpu as pltpu
from jax.sharding import PartitionSpec as P

LANES = 128
TOP = 32767.0
TINY = 1e-30


def largest_tile(columns, most):
    tile = most
    while columns % tile:
        tile //= 2
    return tile


def kernel(dims, hidden, weight, targets, segment, mask, outside, loss_out, sample_out,
           hx, wbuf, ybuf, prt, qs, qr, ss, sr, scale_buf, tg, tcol, m_buf, s_buf, p_buf,
           stat, statr, samp, wsem, local_sem, hsem, csem_s, csem_r, fsem_s, fsem_r, tsem,
           ysem, prsem, qssem, qrsem, sssem, srsem, stsem, strsem, spsem, sprsem):
    dp, nv, rows, depth, tiles, tile, chunks = dims
    chips = dp // 2
    me, v = lax.axis_index("dp"), lax.axis_index("vocab")
    x, c = me // 2, me % 2
    partner = 2 * x + (1 - c)
    owner = 2 * lax.rem(x + 1, chips) + c
    source = 2 * lax.rem(x + chips - 1, chips) + c
    share = rows // chunks

    def remote(src, dst, send, recv, d, w):
        return pltpu.make_async_remote_copy(
            src_ref=src, dst_ref=dst, send_sem=send, recv_sem=recv,
            device_id=(d, w), device_id_type=pl.DeviceIdType.MESH)

    def wcopy(t, slot):
        return pltpu.make_async_copy(
            weight.at[:, pl.ds(pl.multiple_of(t * tile, tile), tile)], wbuf.at[slot], wsem.at[slot])

    def features(d):
        return pl.ds(pl.multiple_of(d * depth, depth), depth)

    def token_rows(d):
        return pl.ds(pl.multiple_of(d * rows, rows), rows)

    def chunk_rows(d, j):
        return pl.ds(pl.multiple_of(d * rows + j * share, share), share)

    wcopy(0, 0).start()
    own = pltpu.make_async_copy(hidden.at[:, features(me)], hx.at[token_rows(me)], local_sem)
    own.start()

    barrier = pltpu.get_barrier_semaphore()

    def greet(d, w):
        pl.semaphore_signal(barrier, inc=1, device_id=(d, w), device_id_type=pl.DeviceIdType.MESH)

    for o in range(1, dp):
        greet(lax.rem(me + o, dp), v)

    columns_met = [0, 1] if chips == 2 else [0, 1, chips - 1]

    def greet_vocab(o, carry):
        w = lax.rem(v + o, nv)
        for step in columns_met:
            greet(2 * lax.rem(x + step, chips) + c, w)
        return carry

    lax.fori_loop(1, nv, greet_vocab, 0)
    pl.semaphore_wait(barrier, dp - 1 + (nv - 1) * len(columns_met))

    to_partner = remote(hidden.at[:, features(partner)], hx.at[token_rows(me)],
                        hsem.at[0], hsem.at[1], partner, v)
    to_partner.start()
    targets_copy = remote(targets, tg, tsem.at[0], tsem.at[1], source, v)

    def crossing(step, e):
        d = 2 * lax.rem(x + step, chips) + e
        src = hidden.at[pl.ds(pl.multiple_of(v * share, share), share), features(d)]
        i = 2 * (step - 1) + e
        r = 2 * (chips - step - 1) + c
        return d, src, i, r

    def cross_start():
        for step in range(1, chips):
            for e in range(2):
                d, src, i, r = crossing(step, e)
                remote(src, hx.at[chunk_rows(me, v)], csem_s.at[i], csem_r.at[r], d, v).start()

    if chunks < nv:
        pl.when(v < chunks)(cross_start)
    else:
        cross_start()
    targets_copy.start()

    def spread_each(step, e, do):
        d = 2 * lax.rem(x + step, chips) + e
        i = 2 * (step - 1) + e

        def one(o, carry):
            w = lax.rem(v + o, nv)
            block = hx.at[chunk_rows(d, v)]
            copy = remote(block, block, fsem_s.at[i, o - 1], fsem_r.at[i, v], me, w)
            do(copy)
            return carry

        lax.fori_loop(1, nv, one, 0)

    def spread():
        for step in range(1, chips):
            for e in range(2):
                d = 2 * lax.rem(x + step, chips) + e
                i = 2 * (step - 1) + e
                block = hx.at[chunk_rows(d, v)]
                remote(block, block, csem_s.at[i], csem_r.at[i], d, v).wait_recv()
                spread_each(step, e, lambda copy: copy.start())

    def spread_wait(step):
        for e in range(2):
            d = 2 * lax.rem(x + step, chips) + e
            i = 2 * (step - 1) + e

            def one(j, carry):
                @pl.when(j != v)
                def _():
                    block = hx.at[chunk_rows(d, j)]
                    remote(block, block, fsem_s.at[i, 0], fsem_r.at[i, j], me, lax.rem(v + 1, nv)).wait_recv()
                return carry

            lax.fori_loop(0, chunks, one, 0)

    def dot_tile(group, slot, yslot):
        width = min(tile, 512)
        lhs_rows = pl.ds(pl.multiple_of(group * 2 * rows, 2 * rows), 2 * rows)

        def piece(j, carry):
            cols = pl.ds(pl.multiple_of(j * width, width), width)
            ybuf[yslot, :, cols] = jnp.dot(hx[lhs_rows, :], wbuf[slot, :, cols],
                                           preferred_element_type=jnp.float32)
            return carry

        lax.fori_loop(0, tile // width, piece, 0)

    def ycopy(s, t, yslot):
        half = pl.ds(pl.multiple_of((1 - c) * rows, rows), rows)
        return remote(ybuf.at[yslot, half], prt.at[s, t], ysem.at[yslot], prsem.at[s, t], partner, v)

    def qcopy(s, t):
        d = 2 * lax.rem(x + chips - s - 1 + chips, chips) + c
        return (remote(qs.at[s, t], qr.at[s, t], qssem.at[s, t], qrsem.at[s, t], d, v),
                remote(ss.at[s, t], sr.at[s, t], sssem.at[s, t], srsem.at[s, t], d, v))

    band = min(rows, 32)

    def total(s, t, yslot, b):
        mine = pl.ds(pl.multiple_of(c * rows + b * band, band), band)
        theirs = pl.ds(b * band, band)
        return ybuf[yslot, mine, :] + prt[s, t, theirs, :]

    def send_sums(s, t, yslot):
        ycopy(s, t, yslot).wait_recv()
        for b in range(rows // band):
            value = total(s, t, yslot, b)
            top = jnp.maximum(jnp.max(jnp.abs(value), axis=1, keepdims=True), TINY)
            code = jnp.round(value * (TOP / top)).astype(jnp.int32)
            qs[s, t, b * band:(b + 1) * band, :] = code.astype(jnp.int16)
            scale_buf[b * band:(b + 1) * band, :] = jnp.broadcast_to(top * (1.0 / TOP), (band, LANES))
        ss[s, t] = jnp.transpose(scale_buf[0:rows, :])[0:8, :]
        for copy in qcopy(s, t):
            copy.start()

    def finish(s, t, yslot):
        ycopy(s, t, yslot).wait_recv()
        for a in range(chips - 1):
            for copy in qcopy(a, t):
                copy.wait_recv()
            scale_buf[a * rows:(a + 1) * rows, :] = jnp.transpose(
                jnp.broadcast_to(sr[a, t, 0:1, :], (LANES, rows)))
        base = v * (tiles * tile) + t * tile
        lane = lax.broadcasted_iota(jnp.int32, (band, LANES), 1)
        for b in range(rows // band):
            here = slice(b * band, (b + 1) * band)
            value = total(s, t, yslot, b)
            parts = []
            for k in range(tile // LANES):
                part = value[:, k * LANES:(k + 1) * LANES]
                for a in range(chips - 1):
                    code = qr[a, t, here, k * LANES:(k + 1) * LANES].astype(jnp.int32)
                    part = part + code.astype(jnp.float32) * scale_buf[a * rows + b * band:a * rows + (b + 1) * band, :]
                parts.append(part)
            old = m_buf[here, :]
            new = functools.reduce(jnp.maximum, parts, old)
            acc = s_buf[here, :] * jnp.exp(old - new)
            picked = p_buf[here, :]
            wanted = tcol[here, :] - base
            for k, part in enumerate(parts):
                acc = acc + jnp.exp(part - new)
                picked = picked + jnp.where(lane + k * LANES == wanted, part, 0.0)
            m_buf[here, :] = new
            s_buf[here, :] = acc
            p_buf[here, :] = picked

    own.wait()
    to_partner.wait_recv()
    m_buf[...] = jnp.full(m_buf.shape, -jnp.inf, jnp.float32)
    s_buf[...] = jnp.zeros(s_buf.shape, jnp.float32)
    p_buf[...] = jnp.zeros(p_buf.shape, jnp.float32)

    for s in range(chips):
        group = lax.rem(x + chips - s, chips)
        last = s == chips - 1
        if s > 0:
            spread_wait(chips - s)
        if last:
            targets_copy.wait_recv()
            tcol[...] = jnp.transpose(jnp.broadcast_to(tg[0:1, :], (LANES, rows)))
        handle = finish if last else send_sums

        def step(t, carry, s=s, group=group, last=last, handle=handle):
            i = s * tiles + t
            slot = lax.rem(i, 2)
            wcopy(t, slot).wait()

            @pl.when(i + 1 < chips * tiles)
            def _():
                wcopy(lax.rem(t + 1, tiles), 1 - slot).start()

            @pl.when(i >= 2)
            def _():
                ycopy(s, t, slot).wait_send()

            dot_tile(group, slot, slot)
            ycopy(s, t, slot).start()

            @pl.when(t >= 1)
            def _():
                handle(s, t - 1, 1 - slot)

            if s == 0:
                @pl.when(t == min(1, tiles - 1))
                def _():
                    if chunks < nv:
                        pl.when(v < chunks)(spread)
                    else:
                        spread()
            return carry

        lax.fori_loop(0, tiles, step, 0)
        handle(s, tiles - 1, (s * tiles + tiles - 1) % 2)

    lane = lax.broadcasted_iota(jnp.int32, (rows, LANES), 1)
    peak = jnp.max(m_buf[...], axis=1, keepdims=True)
    mass = jnp.sum(s_buf[...] * jnp.exp(m_buf[...] - peak), axis=1, keepdims=True)
    hit = jnp.sum(p_buf[...], axis=1, keepdims=True)
    table = jnp.where(lane == 0, peak, jnp.where(lane == 1, mass, hit))
    stat[...] = jnp.transpose(table)[0:8, :]

    def stat_copy(w):
        return remote(stat, statr.at[v], stsem.at[w], strsem.at[v], owner, w)

    def stat_start(o, carry):
        stat_copy(lax.rem(v + o, nv)).start()
        return carry

    lax.fori_loop(0, nv, stat_start, 0)

    def stat_wait(w, carry):
        remote(stat, statr.at[w], stsem.at[w], strsem.at[w], owner, w).wait_recv()
        return carry

    lax.fori_loop(0, nv, stat_wait, 0)
    peak = statr[0, 0:1, :]
    for w in range(1, nv):
        peak = jnp.maximum(peak, statr[w, 0:1, :])
    mass = jnp.zeros_like(peak)
    hit = jnp.zeros_like(peak)
    for w in range(nv):
        mass = mass + statr[w, 1:2, :] * jnp.exp(statr[w, 0:1, :] - peak)
        hit = hit + statr[w, 2:3, :]
    loss = peak + jnp.log(mass) - hit
    loss_out[...] = loss

    samples = outside.shape[0]
    weights = mask[...].astype(jnp.float32)
    member = lax.broadcasted_iota(jnp.int32, (samples, rows), 0) == segment[...]
    sums = jnp.sum(jnp.where(member, loss * weights, 0.0), axis=1, keepdims=True)
    count = jnp.sum(jnp.where(member, weights, 0.0), axis=1, keepdims=True)
    wide = lax.broadcasted_iota(jnp.int32, (samples, LANES), 1)
    samp[me] = jnp.where(wide < LANES // 2, sums, count)

    def samp_copy(o, d):
        return remote(samp.at[d], samp.at[d], spsem.at[o - 1], sprsem.at[d], lax.rem(me + o, dp), v)

    for o in range(1, dp):
        samp_copy(o, me).start()
    for o in range(1, dp):
        samp_copy(o, lax.rem(me + o, dp)).wait_recv()
    both = samp[0]
    for d in range(1, dp):
        both = both + samp[d]
    sums = both[:, 0:1]
    count = both[:, LANES - 1:LANES]
    denom = jnp.maximum(count + outside[...].astype(jnp.float32), 1.0)
    sample_out[...] = sums / denom

    to_partner.wait_send()
    targets_copy.wait_send()

    def leave():
        for step in range(1, chips):
            for e in range(2):
                d, src, i, r = crossing(step, e)
                remote(src, hx.at[chunk_rows(me, v)], csem_s.at[i], csem_r.at[r], d, v).wait_send()
                spread_each(step, e, lambda copy: copy.wait_send())

    if chunks < nv:
        pl.when(v < chunks)(leave)
    else:
        leave()
    for k in range(min(2, chips * tiles)):
        ycopy(0, 0, k).wait_send()

    def sums_left(t, carry):
        for s in range(chips - 1):
            for copy in qcopy(s, t):
                copy.wait_send()
        return carry

    lax.fori_loop(0, tiles, sums_left, 0)

    def stat_left(w, carry):
        stat_copy(w).wait_send()
        return carry

    lax.fori_loop(0, nv, stat_left, 0)
    for o in range(1, dp):
        samp_copy(o, me).wait_send()


def solution(mesh):
    dp, nv = mesh.shape["dp"], mesh.shape["vocab"]

    def body(hidden, out_weight, targets, segment, loss_mask, outside_count):
        rows = hidden.shape[0]
        depth, columns = out_weight.shape
        samples = outside_count.shape[0]
        chips = dp // 2
        tile = largest_tile(columns, 1024)
        tiles = columns // tile
        chunks = min(nv, rows // 16)
        dims = (dp, nv, rows, depth, tiles, tile, chunks)
        sem = pltpu.SemaphoreType.DMA
        far = 2 * (chips - 1)
        vm = pl.BlockSpec(memory_space=pltpu.VMEM)
        hbm = pl.BlockSpec(memory_space=pl.ANY)
        loss, sample = pl.pallas_call(
            functools.partial(kernel, dims),
            out_shape=(jax.ShapeDtypeStruct((1, rows), jnp.float32),
                       jax.ShapeDtypeStruct((samples, LANES), jnp.float32)),
            in_specs=[hbm, hbm, vm, vm, vm, vm],
            out_specs=(vm, vm),
            scratch_shapes=[
                pltpu.VMEM((dp * rows, depth), jnp.bfloat16),
                pltpu.VMEM((2, depth, tile), jnp.bfloat16),
                pltpu.VMEM((2, 2 * rows, tile), jnp.float32),
                pltpu.VMEM((chips, tiles, rows, tile), jnp.float32),
                pltpu.VMEM((chips - 1, tiles, rows, tile), jnp.int16),
                pltpu.VMEM((chips - 1, tiles, rows, tile), jnp.int16),
                pltpu.VMEM((chips - 1, tiles, 8, rows), jnp.float32),
                pltpu.VMEM((chips - 1, tiles, 8, rows), jnp.float32),
                pltpu.VMEM(((chips - 1) * rows, LANES), jnp.float32),
                pltpu.VMEM((8, rows), jnp.int32),
                pltpu.VMEM((rows, LANES), jnp.int32),
                pltpu.VMEM((rows, LANES), jnp.float32),
                pltpu.VMEM((rows, LANES), jnp.float32),
                pltpu.VMEM((rows, LANES), jnp.float32),
                pltpu.VMEM((8, rows), jnp.float32),
                pltpu.VMEM((nv, 8, rows), jnp.float32),
                pltpu.VMEM((dp, samples, LANES), jnp.float32),
                sem((2,)), sem, sem((2,)), sem((far,)), sem((far,)),
                sem((far, nv - 1)), sem((far, chunks)), sem((2,)),
                sem((2,)), sem((chips, tiles)),
                sem((chips - 1, tiles)), sem((chips - 1, tiles)),
                sem((chips - 1, tiles)), sem((chips - 1, tiles)),
                sem((nv,)), sem((nv,)), sem((dp - 1,)), sem((dp,)),
            ],
            compiler_params=pltpu.CompilerParams(
                collective_id=0, has_side_effects=True, vmem_limit_bytes=60 * 1024 * 1024),
        )(hidden, out_weight,
          jnp.broadcast_to(targets[None, :], (8, rows)),
          segment[None, :], loss_mask[None, :],
          jnp.broadcast_to(outside_count[:, None], (samples, LANES)))
        return loss[0], sample[:, 0]

    return jax.shard_map(
        body,
        mesh=mesh,
        in_specs=(P("dp", None), P("dp", "vocab"), P("dp"), P("dp"), P("dp"), P()),
        out_specs=(P("dp"), P()),
        check_vma=False,
    )
```
